32 devices in a mesh: row: 4 (over z), col: 2 (over y), layer: 4 (over x, core).
Axes of the slice: x: 2, y: 2, z: 4, core: 2. Of those that a mesh axis runs over, the one named last changes fastest.
Arguments:
- amplitudes: float32 [2016, 73536], P('row', ('layer', 'col')), may hold values from -6 to 6
- integrals: float32 [73536, 768], P(('layer', 'col'), 'row'), may hold values from -0.03125 to 0.03125
- occ_energy: float32 [64], replicated, may hold values from -2 to -0.5
- vir_energy: float32 [384], replicated, may hold values from 0.2 to 3
Outputs:
- ladder: float32 [2016, 768], P('col', ('row', 'layer'))
- amplitude_step: float32 [2016, 768], P('col', ('row', 'layer'))
The draws below stay inside these ranges and needn't reach their ends.
All inputs are finite; a program needn't handle non-finite values.
Results may differ from the reference program's by a relative error of at most 0.00007.
Values sent between devices are 32-bit elements; how exact they have to be, the bound alone decides.
A program may use at most 128 MiB of HBM per device.

```python
import jax
import jax.numpy as jnp
import numpy as np
from jax import lax

NO = 64
NV = 384
IJ = 2016
K = 73536
AB = 768


def spiked(values, stream_key, source, target, parts, factor):
    def block_of(dim):
        return (jnp.arange(values.shape[dim]) // (values.shape[dim] // parts)).reshape((-1,) + (1,) * (values.ndim - 1 - dim))

    one_side = jax.random.permutation(stream_key, parts)[block_of(target)]
    far = (block_of(target) + parts // 2) % parts
    return jnp.where((block_of(source) == one_side) | (block_of(source) == far), factor * values, values)


def level_of(stream_key, shape, pieces, low, top_value):
    level, own = 1.0, jax.random.fold_in(stream_key, 6)
    for axis_at, parts in pieces:
        steps = jnp.exp(jax.random.uniform(jax.random.fold_in(own, axis_at), (parts,), jnp.float32, low / len(pieces), top_value / len(pieces)))
        level = level * jnp.repeat(steps, shape[axis_at] // parts).reshape([-1 if axis == axis_at else 1 for axis in range(len(shape))])
    return level


def gaussian(own_key, shape, deviation, limit, shards=(), kind=jnp.bfloat16):
    result = jax.random.normal(own_key, shape, jnp.float32) * deviation
    if len(shards) > 0:
        result = level_of(own_key, shape, shards, -0.22, 0.18) * result
    return jnp.clip(result, min=-limit, max=limit).astype(kind)


def noise_with(key, shape, deviation, reach, split, heavy, kind=jnp.bfloat16):
    values = deviation * jax.random.normal(key, shape, jnp.float32)
    if split:
        values = values * level_of(key, shape, split, -0.22, 0.18)
    return jnp.clip(spiked(values, jax.random.fold_in(key, 3), *heavy), -reach, reach).astype(kind)


def setup_inputs(seed: int = 0) -> dict:
    seeds = jax.random.split(jax.random.key(seed), 5)
    return {
        "amplitudes": gaussian(seeds[0], (IJ, K), 1.0, 6.0, ((0, 4), (1, 8)), jnp.float32),
        "integrals": noise_with(seeds[1], (K, AB), K ** -0.5, 0.03125, ((0, 8), (1, 4)), (0, 1, 8, 2.0), jnp.float32),
        "occ_energy": jnp.clip(jax.random.uniform(seeds[2], (NO,), jnp.float32, -2.0, -0.5), -2.0, -0.5),
        "vir_energy": jnp.clip(jax.random.uniform(seeds[3], (NV,), jnp.float32, 0.2, 3.0), 0.2, 3.0),
    }


def reference(amplitudes, integrals, occ_energy, vir_energy):
    first_np, second_np = np.triu_indices(NO, 1)
    first_index = jnp.asarray(first_np, dtype=jnp.int32)
    second_index = jnp.asarray(second_np, dtype=jnp.int32)
    ladder = jnp.dot(amplitudes, integrals, precision=lax.Precision.HIGHEST, preferred_element_type=jnp.float32)
    pair_sum = occ_energy[first_index] + occ_energy[second_index]
    ab_index = jnp.arange(AB, dtype=jnp.int32)
    vir_sum = vir_energy[ab_index // NV] + vir_energy[ab_index % NV]
    denominator = pair_sum[:, None] - vir_sum[None, :]
    return ladder, ladder / denominator
```

```python
import jax
import jax.numpy as jnp
import numpy as np
from jax import lax
from jax.sharding import PartitionSpec as P


def lookup(indices, values_table):
    positions = jnp.arange(values_table.shape[0], dtype=jnp.int32)
    picked = jnp.where(indices[:, None] == positions[None, :], values_table[None, :], 0.0)
    return jnp.sum(picked, axis=1)


def owner_blocks(partial_sum):
    col_count = lax.axis_size("col")
    layer_count = lax.axis_size("layer")
    pair_rows = partial_sum.shape[0] // col_count
    slab_cols = partial_sum.shape[1] // layer_count
    blocks = partial_sum.reshape(col_count, pair_rows, layer_count, slab_cols)
    return blocks.transpose(0, 2, 1, 3).reshape(col_count * layer_count * pair_rows, slab_cols)


def contract(columns, rows):
    return lax.dot_general(
        columns,
        rows,
        (((1,), (1,)), ((), ())),
        precision=lax.Precision.HIGH,
        preferred_element_type=jnp.float32,
    )


def near_depth(depth):
    return -(-depth // (6 * 128)) * 128


def settled(value):
    return lax.optimization_barrier(value)


def line_exchange(amplitudes, integrals):
    row = lax.axis_index("row")
    low = row < 2
    edge = (row == 0) | (row == 3)
    pair_rows = amplitudes.shape[0]
    depth, width = integrals.shape
    near = near_depth(depth)
    far = 2 * near
    columns = integrals.T
    parts = [0, far + near]
    firsts = [columns[:, start : start + far] for start in parts]
    up_pairs = [(0, 1), (1, 2), (2, 3)]
    down_pairs = [(3, 2), (2, 1), (1, 0)]

    def shift(up_payload, down_payload):
        return (
            lax.ppermute(up_payload, "row", up_pairs),
            lax.ppermute(down_payload, "row", down_pairs),
        )

    def sides(pair):
        up, down = pair
        return jnp.where(low, down, up), jnp.where(low, up, down)

    def kept(value):
        return jnp.where(edge, 0.0, value)

    hop1 = [shift(first, first) for first in firsts]
    seconds = []
    shared = []
    for start in parts:
        end = min(start + far + near, depth)
        pad = start + far + near - end
        seconds.append(jnp.pad(columns[:, start + far : end], ((0, 0), (0, pad))))
        shared.append(
            jnp.pad(amplitudes[:, start + far : end], ((0, 3 * width - pair_rows), (0, pad)))
        )
    hop2 = []
    for part in range(2):
        up1, down1 = hop1[part]
        edge2 = jnp.concatenate([seconds[part], shared[part][:width]], axis=1)
        hop2.append(
            shift(jnp.where(row == 0, edge2, up1), jnp.where(row == 3, edge2, down1))
        )
    hop3 = []
    for part in range(2):
        up2, down2 = hop2[part]
        edge3 = jnp.concatenate(
            [shared[part][width : 2 * width], shared[part][2 * width :]], axis=1
        )
        up_mid = jnp.concatenate([seconds[part], up2[:, :near]], axis=1)
        down_mid = jnp.concatenate([seconds[part], down2[:, :near]], axis=1)
        hop3.append(
            shift(
                jnp.where(row == 0, edge3, jnp.where(row == 1, up_mid, up2)),
                jnp.where(row == 3, edge3, jnp.where(row == 2, down_mid, down2)),
            )
        )
    own = settled(contract(columns, amplitudes))
    slot1 = slot2 = slot3 = extra1 = extra2 = extra3 = 0.0
    for part, start in enumerate(parts):
        rows_first = amplitudes[:, start : start + far]
        own_rows = shared[part][:pair_rows]
        inner1, outer1 = sides(hop1[part])
        slot1 += settled(contract(inner1, rows_first))
        third = settled(contract(outer1, rows_first))
        inner2, outer2 = sides(hop2[part])
        slot2 += settled(contract(inner2, rows_first))
        third = settled(third + contract(outer2[:, :near], own_rows))
        inner3, outer3 = sides(hop3[part])
        last = settled(contract(inner3, rows_first))
        slot3 += jnp.where(edge, last, third)
        columns3 = jnp.concatenate([inner3[:, :near], inner3[:, near:]], axis=0)
        columns3 = kept(columns3)
        mixed = settled(contract(columns3, own_rows))
        slot1 += mixed[:width]
        slot2 += mixed[width:]
        sent = jnp.concatenate([outer2[:, near:], outer3[:, :near], outer3[:, near:]], axis=0)
        sent = kept(sent[:pair_rows])
        three = settled(contract(jnp.concatenate([seconds[part], columns3], axis=0), sent))
        extra1 += three[:width]
        extra2 += three[width : 2 * width]
        extra3 += three[2 * width :]

    slots = [own, slot1, slot2, slot3]
    order = [jnp.where(edge, slots[at], slots[(at + 3) % 4]) for at in range(4)]
    extra = [jnp.zeros_like(extra1), extra1, extra2, extra3]
    both = [jnp.stack([order[at], extra[at]]) for at in range(4)]
    both = [jnp.where(low, both[at], both[3 - at]) for at in range(4)]
    layers = lax.axis_size("layer")
    slab = width // layers
    stacked = jnp.stack(both).reshape(2, 2, 2, layers, slab, pair_rows)
    stacked = stacked.transpose(0, 3, 1, 2, 4, 5).reshape(-1, 2, 2, slab, pair_rows)
    mine = lax.psum_scatter(stacked, ("col", "layer"), scatter_dimension=0, tiled=True)[0]
    odd = row % 2 == 1
    same = jnp.where(odd, mine[1], mine[0])
    other = jnp.where(odd, mine[0], mine[1])
    same_pairs = []
    other_pairs = []
    for source_row in range(4):
        for source_col in range(2):
            bit = source_row % 2
            source = source_row * 2 + source_col
            same_pairs.append((source, (2 * source_col + bit) * 2 + source_row // 2))
            other_pairs.append((source, (2 * source_col + 1 - bit) * 2 + source_row // 2))
    same = lax.ppermute(same, ("row", "col"), same_pairs)
    other = lax.ppermute(other, ("row", "col"), other_pairs)
    even_rows = jnp.where(odd, other, same)
    odd_rows = jnp.where(odd, same, other)
    return jnp.concatenate([even_rows[0] + odd_rows[1], odd_rows[0] + even_rows[1]], axis=1)


def gathered(amplitudes, integrals):
    partial_rows = jnp.dot(
        amplitudes,
        lax.all_gather(integrals, "row", axis=1, tiled=True),
        precision=lax.Precision.HIGHEST,
        preferred_element_type=jnp.float32,
    )
    partial_sum = lax.all_to_all(partial_rows, "row", split_axis=1, concat_axis=0, tiled=True)
    return lax.psum_scatter(
        owner_blocks(partial_sum), ("col", "layer"), scatter_dimension=0, tiled=True
    )


def shards(amplitudes, integrals, occ_energy, vir_energy):
    in_line = lax.axis_size("row") == 4 and lax.axis_size("col") == 2
    fits = amplitudes.shape[0] <= 3 * integrals.shape[1]
    depth = integrals.shape[0]
    if in_line and fits and depth > 5 * near_depth(depth):
        ladder = line_exchange(amplitudes, integrals).T
    else:
        ladder = gathered(amplitudes, integrals)
    pair_rows = ladder.shape[0]
    slab_cols = ladder.shape[1]
    occupied = occ_energy.shape[0]
    virtuals = vir_energy.shape[0]
    first_np, second_np = np.triu_indices(occupied, 1)
    ij_start = lax.axis_index("col") * pair_rows
    ab_start = (
        lax.axis_index("row") * lax.axis_size("layer") + lax.axis_index("layer")
    ) * slab_cols
    first_index = lax.dynamic_slice_in_dim(
        jnp.asarray(first_np, dtype=jnp.int32), ij_start, pair_rows
    )
    second_index = lax.dynamic_slice_in_dim(
        jnp.asarray(second_np, dtype=jnp.int32), ij_start, pair_rows
    )
    pair_sum = lookup(first_index, occ_energy) + lookup(second_index, occ_energy)
    ab_index = ab_start + jnp.arange(slab_cols, dtype=jnp.int32)
    vir_sum = lookup(ab_index // virtuals, vir_energy) + lookup(ab_index % virtuals, vir_energy)
    denominator = pair_sum[:, None] - vir_sum[None, :]
    return (ladder, ladder / denominator)


def solution(mesh):
    in_specs = (P("row", ("layer", "col")), P(("layer", "col"), "row"), P(), P())
    out_specs = (P("col", ("row", "layer")), P("col", ("row", "layer")))
    return jax.shard_map(shards, mesh=mesh, in_specs=in_specs, out_specs=out_specs, check_vma=False)
```

```python
import jax
import jax.numpy as jnp
import numpy as np
from jax import lax
from jax.sharding import PartitionSpec as P


def lookup(indices, values_table):
    positions = jnp.arange(values_table.shape[0], dtype=jnp.int32)
    picked = jnp.where(indices[:, None] == positions[None, :], values_table[None, :], 0.0)
    return jnp.sum(picked, axis=1)


def owner_blocks(partial_sum):
    col_count = lax.axis_size("col")
    layer_count = lax.axis_size("layer")
    pair_rows = partial_sum.shape[0] // col_count
    slab_cols = partial_sum.shape[1] // layer_count
    blocks = partial_sum.reshape(col_count, pair_rows, layer_count, slab_cols)
    return blocks.transpose(0, 2, 1, 3).reshape(col_count * layer_count * pair_rows, slab_cols)


def contract(columns, rows):
    return lax.dot_general(
        columns,
        rows,
        (((1,), (1,)), ((), ())),
        precision=lax.Precision.HIGH,
        preferred_element_type=jnp.float32,
    )


def near_depth(depth):
    return -(-depth // (6 * 128)) * 128


def settled(value):
    return lax.optimization_barrier(value)


def halves(blocks, dim, upper, axis, swap):
    low_half = lax.index_in_dim(blocks, 0, dim, keepdims=False)
    high_half = lax.index_in_dim(blocks, 1, dim, keepdims=False)
    given = jnp.where(upper, low_half, high_half)
    return jnp.where(upper, high_half, low_half) + lax.ppermute(given, axis, swap)


def line_exchange(amplitudes, integrals):
    row = lax.axis_index("row")
    low = row < 2
    edge = (row == 0) | (row == 3)
    pair_rows = amplitudes.shape[0]
    depth, width = integrals.shape
    near = near_depth(depth)
    far = 2 * near
    columns = integrals.T
    parts = [0, far + near]
    firsts = [columns[:, start : start + far] for start in parts]
    up_pairs = [(0, 1), (1, 2), (2, 3)]
    down_pairs = [(3, 2), (2, 1), (1, 0)]

    def shift(up_payload, down_payload):
        return (
            lax.ppermute(up_payload, "row", up_pairs),
            lax.ppermute(down_payload, "row", down_pairs),
        )

    def sides(pair):
        up, down = pair
        return jnp.where(low, down, up), jnp.where(low, up, down)

    def kept(value):
        return jnp.where(edge, 0.0, value)

    hop1 = [shift(first, first) for first in firsts]
    seconds = []
    shared = []
    for start in parts:
        end = min(start + far + near, depth)
        pad = start + far + near - end
        seconds.append(jnp.pad(columns[:, start + far : end], ((0, 0), (0, pad))))
        shared.append(
            jnp.pad(amplitudes[:, start + far : end], ((0, 3 * width - pair_rows), (0, pad)))
        )
    hop2 = []
    for part in range(2):
        up1, down1 = hop1[part]
        edge2 = jnp.concatenate([seconds[part], shared[part][:width]], axis=1)
        hop2.append(
            shift(jnp.where(row == 0, edge2, up1), jnp.where(row == 3, edge2, down1))
        )
    hop3 = []
    for part in range(2):
        up2, down2 = hop2[part]
        edge3 = jnp.concatenate(
            [shared[part][width : 2 * width], shared[part][2 * width :]], axis=1
        )
        up_mid = jnp.concatenate([seconds[part], up2[:, :near]], axis=1)
        down_mid = jnp.concatenate([seconds[part], down2[:, :near]], axis=1)
        hop3.append(
            shift(
                jnp.where(row == 0, edge3, jnp.where(row == 1, up_mid, up2)),
                jnp.where(row == 3, edge3, jnp.where(row == 2, down_mid, down2)),
            )
        )
    own = settled(contract(columns, amplitudes))
    slot1 = slot2 = slot3 = extra1 = extra2 = extra3 = 0.0
    for part, start in enumerate(parts):
        rows_first = amplitudes[:, start : start + far]
        own_rows = shared[part][:pair_rows]
        inner1, outer1 = sides(hop1[part])
        slot1 += settled(contract(inner1, rows_first))
        third = settled(contract(outer1, rows_first))
        inner2, outer2 = sides(hop2[part])
        slot2 += settled(contract(inner2, rows_first))
        third = settled(third + contract(outer2[:, :near], own_rows))
        inner3, outer3 = sides(hop3[part])
        last = settled(contract(inner3, rows_first))
        slot3 += jnp.where(edge, last, third)
        columns3 = jnp.concatenate([inner3[:, :near], inner3[:, near:]], axis=0)
        columns3 = kept(columns3)
        mixed = settled(contract(columns3, own_rows))
        slot1 += mixed[:width]
        slot2 += mixed[width:]
        sent = jnp.concatenate([outer2[:, near:], outer3[:, :near], outer3[:, near:]], axis=0)
        sent = kept(sent[:pair_rows])
        three = settled(contract(jnp.concatenate([seconds[part], columns3], axis=0), sent))
        extra1 += three[:width]
        extra2 += three[width : 2 * width]
        extra3 += three[2 * width :]

    slots = [own, slot1, slot2, slot3]
    order = [jnp.where(edge, slots[at], slots[(at + 3) % 4]) for at in range(4)]
    extra = [jnp.zeros_like(extra1), extra1, extra2, extra3]
    both = [jnp.stack([order[at], extra[at]]) for at in range(4)]
    both = [jnp.where(low, both[at], both[3 - at]) for at in range(4)]
    layers = lax.axis_size("layer")
    slab = width // layers
    stacked = jnp.stack(both).reshape(2, 2, 2, 2, 2, slab, pair_rows)
    layer = lax.axis_index("layer")
    upper_col = lax.axis_index("col") == 1
    upper_pair = layer // 2 == 1
    pair_swap = [(0, 2), (2, 0), (1, 3), (3, 1)]
    core_swap = [(0, 1), (1, 0), (2, 3), (3, 2)]
    col_swap = [(0, 1), (1, 0)]
    halved = halves(stacked, 4, layer % 2 == 1, "layer", core_swap)
    pair_first = halves(halved[:, 0], 2, upper_pair, "layer", pair_swap)
    col_first = halves(halved[:, 1], 0, upper_col, "col", col_swap)
    mine = (
        halves(pair_first, 0, upper_col, "col", col_swap),
        halves(col_first, 1, upper_pair, "layer", pair_swap),
    )
    odd = row % 2 == 1
    same = jnp.where(odd, mine[1], mine[0])
    other = jnp.where(odd, mine[0], mine[1])
    same_pairs = []
    other_pairs = []
    for source_row in range(4):
        for source_col in range(2):
            bit = source_row % 2
            source = source_row * 2 + source_col
            same_pairs.append((source, (2 * source_col + bit) * 2 + source_row // 2))
            other_pairs.append((source, (2 * source_col + 1 - bit) * 2 + source_row // 2))
    same = lax.ppermute(same, ("row", "col"), same_pairs)
    other = lax.ppermute(other, ("row", "col"), other_pairs)
    even_rows = jnp.where(odd, other, same)
    odd_rows = jnp.where(odd, same, other)
    return jnp.concatenate([even_rows[0] + odd_rows[1], odd_rows[0] + even_rows[1]], axis=1)


def gathered(amplitudes, integrals):
    partial_rows = jnp.dot(
        amplitudes,
        lax.all_gather(integrals, "row", axis=1, tiled=True),
        precision=lax.Precision.HIGHEST,
        preferred_element_type=jnp.float32,
    )
    partial_sum = lax.all_to_all(partial_rows, "row", split_axis=1, concat_axis=0, tiled=True)
    return lax.psum_scatter(
        owner_blocks(partial_sum), ("col", "layer"), scatter_dimension=0, tiled=True
    )


def shards(amplitudes, integrals, occ_energy, vir_energy):
    in_line = lax.axis_size("row") == 4 and lax.axis_size("col") == 2
    in_line = in_line and lax.axis_size("layer") == 4
    fits = amplitudes.shape[0] <= 3 * integrals.shape[1]
    depth = integrals.shape[0]
    if in_line and fits and depth > 5 * near_depth(depth):
        ladder = line_exchange(amplitudes, integrals).T
    else:
        ladder = gathered(amplitudes, integrals)
    pair_rows = ladder.shape[0]
    slab_cols = ladder.shape[1]
    occupied = occ_energy.shape[0]
    virtuals = vir_energy.shape[0]
    first_np, second_np = np.triu_indices(occupied, 1)
    ij_start = lax.axis_index("col") * pair_rows
    ab_start = (
        lax.axis_index("row") * lax.axis_size("layer") + lax.axis_index("layer")
    ) * slab_cols
    first_index = lax.dynamic_slice_in_dim(
        jnp.asarray(first_np, dtype=jnp.int32), ij_start, pair_rows
    )
    second_index = lax.dynamic_slice_in_dim(
        jnp.asarray(second_np, dtype=jnp.int32), ij_start, pair_rows
    )
    pair_sum = lookup(first_index, occ_energy) + lookup(second_index, occ_energy)
    ab_index = ab_start + jnp.arange(slab_cols, dtype=jnp.int32)
    vir_sum = lookup(ab_index // virtuals, vir_energy) + lookup(ab_index % virtuals, vir_energy)
    denominator = pair_sum[:, None] - vir_sum[None, :]
    return (ladder, ladder / denominator)


def solution(mesh):
    in_specs = (P("row", ("layer", "col")), P(("layer", "col"), "row"), P(), P())
    out_specs = (P("col", ("row", "layer")), P("col", ("row", "layer")))
    return jax.shard_map(shards, mesh=mesh, in_specs=in_specs, out_specs=out_specs, check_vma=False)
```
